32 devices in a mesh: fit: 4 (over z), pair: 8 (over y, x, core).
Axes of the slice: x: 2, y: 2, z: 4, core: 2. Of those that a mesh axis runs over, the one named last changes fastest.
Arguments:
- metric_factor: bfloat16 [4096, 4096], P('fit'), as said below
- three_index: bfloat16 [4096, 16384], P('fit', 'pair'), may hold values from -6 to 6
- send_map: int32 [8, 8, 16], P('pair'), may hold values from 0 to 15
- pair_slots: int32 [8, 128], P('pair'), may hold values from 0 to 127, each once within a row
- pair_count: int32 [8], P('pair'), may hold values from 1 to 64, 256 in all
- orbital_energy: bfloat16 [128], P('pair'), may hold values from -2 to -0.19921875
- cabs_energy: float32 [1024], replicated, may hold values from 0.5 to 4
- coupling: bfloat16 [128, 1024], replicated, may hold values from -0.5 to 0.5
Outputs:
- projected: bfloat16 [8, 64, 128, 1024], P('pair', 'fit')
The draws below stay inside these ranges and needn't reach their ends.
Inputs may be any that keep to these rules, and one draw needn't show every extreme that they name: `metric_factor`: diagonal entries lie between 0.6 and 1.4. `pair_slots`: each row holds every position 0 to 127 once; pair n of a row uses entries 2n and 2n + 1.
All inputs are finite; a program needn't handle non-finite values. No bound on the sum of `pair_count` on one device may be relied on, other than what follows from the above.
Results may differ from the reference program's by a relative error of at most 0.015.
Values may be sent and summed in bfloat16 or wider, within the bound.
No kernel may reach another device: no remote copies, remote signals or barrier semaphores. Data moves between devices by JAX's collectives and lax.ppermute only.
A program may use at most 256 MiB of HBM per device.

```python
import math
import jax
import jax.numpy as jnp
import numpy as np
from jax import lax

NAUX = 4096
DOM = 128
NCABS = 1024
LMO_DEV = 16
PAIR_CAP = 64
NLMO = 128
CAP = 16
N_PAIR = 8


def draw_metric_factor(key, part):
    first, second = jax.random.split(jax.random.fold_in(key, 17))
    spread = jax.random.normal(first, (NAUX, NAUX), jnp.float32) * (0.8 / NAUX ** 0.5)
    diagonal = jax.random.uniform(second, (NAUX,), jnp.float32, 0.6, 1.4)
    eye = jnp.eye(NAUX, dtype=jnp.float32)
    factor = spread * (1.0 - eye) + jnp.diag(diagonal)
    return factor.astype(jnp.bfloat16)


def plant(drawn, stream_key, smallest, largest):
    extent = drawn.shape
    place = [jax.random.randint(jax.random.fold_in(stream_key, axis), (), 0, extent[axis]) for axis in range(len(extent))]
    drawn = drawn.at[tuple(place)].set(smallest)
    longest = extent.index(max(extent))
    place[longest] = (place[longest] + 1) % extent[longest]
    return drawn.at[tuple(place)].set(largest)


def shard_levels(rng, shape, pieces, least, high):
    def one(axis_at, blocks):
        draws = jax.random.uniform(jax.random.fold_in(jax.random.fold_in(rng, 6), axis_at), (blocks,), jnp.float32, least / len(pieces), high / len(pieces))
        return jnp.repeat(jnp.exp(draws), shape[axis_at] // blocks).reshape((-1,) + (1,) * (len(shape) - axis_at - 1))

    loudness = one(*pieces[0])
    for cut in pieces[1:]:
        loudness = loudness * one(*cut)
    return loudness


def split_up(number_of, total, limit, lean):
    portions = [(1 << 20) // math.isqrt(rank ** lean) + 1 for rank in range(2, number_of + 1)]
    spare, counts = total - limit - (number_of - 1), [1] * (number_of - 1)
    while spare > 0:
        movable = [i for i in range(number_of - 1) if counts[i] < limit]
        whole, remaining = sum([portions[i] for i in movable]), spare
        for i in movable:
            addition = min(limit - counts[i], max(1, remaining * portions[i] // whole), spare)
            counts[i] = counts[i] + addition
            spare = spare - addition
    return np.array([limit] + counts)


def ragged_sizes(stream_key, amount, total, limit, lean):
    if amount == 2:
        one = jax.random.randint(stream_key, (), max(1, total - limit), min(limit, total - 1) + 1)
        return jnp.stack([one, total - one])
    sizes = jnp.asarray(split_up(amount, total, limit, lean), jnp.int32)
    pairs = (amount - 1) // 2
    giver, sink = sizes[1:1 + 2 * pairs:2], sizes[2:2 + 2 * pairs:2]
    room = jnp.minimum(giver - 1, limit - sink)
    shifted = jax.random.randint(jax.random.fold_in(stream_key, 1), (pairs,), 0, 1 << 20) % (room + 1)
    sizes = sizes.at[1:1 + 2 * pairs:2].set(giver - shifted).at[2:2 + 2 * pairs:2].set(sink + shifted)
    return sizes[jax.random.permutation(jax.random.fold_in(stream_key, 2), amount)]


def scatter_about(own_key, extent, width, bound, cuts=(), kind=jnp.bfloat16):
    factor_of = shard_levels(own_key, extent, cuts, -0.22, 0.18) if cuts else 1.0
    values = jax.random.normal(own_key, extent, jnp.float32) * width * factor_of
    return jnp.minimum(jnp.maximum(values, -bound), bound).astype(kind)


def setup_inputs(seed: int = 0) -> dict:
    key_of = jax.random.split(jax.random.key(seed), 9)
    metric_factor = draw_metric_factor(jax.random.fold_in(key_of[8], 71), 0)
    three_index = scatter_about(key_of[1], (NAUX, NLMO * DOM), 1.0, 6.0, ((0, 4), (1, 8)))
    send_map = plant(jax.random.randint(key_of[2], (N_PAIR, N_PAIR, CAP), 0, LMO_DEV), jax.random.fold_in(key_of[2], 1), 0, LMO_DEV - 1).astype(jnp.int32)
    pair_slots = jax.vmap(lambda own: jax.random.permutation(own, 2 * PAIR_CAP))(jax.random.split(key_of[3], N_PAIR)).reshape((N_PAIR, 2 * PAIR_CAP)).astype(jnp.int32)
    pair_count = ragged_sizes(key_of[4], N_PAIR, PAIR_CAP * N_PAIR // 2, PAIR_CAP, 2).astype(jnp.int32)
    orbital_energy = jnp.clip(-2.0 + 1.8007812 * jax.random.uniform(key_of[5], (NLMO,), jnp.float32) ** shard_levels(key_of[5], (NLMO,), ((0, 8),), -0.2, 0.2), -2.0, -0.19921875).astype(jnp.bfloat16)
    cabs_energy = jnp.clip(jnp.exp(jax.random.uniform(key_of[6], (NCABS,), jnp.float32, math.log(0.5), math.log(4.0))), 0.5, 4.0)
    coupling = scatter_about(key_of[7], (DOM, NCABS), DOM ** -0.5, 0.5)
    return {"metric_factor": metric_factor, "three_index": three_index, "send_map": send_map, "pair_slots": pair_slots, "pair_count": pair_count, "orbital_energy": orbital_energy, "cabs_energy": cabs_energy, "coupling": coupling}


def reference(metric_factor, three_index, send_map, pair_slots, pair_count, orbital_energy, cabs_energy, coupling):
    fitted = jnp.dot(metric_factor, three_index, preferred_element_type=jnp.float32).astype(jnp.bfloat16)
    fitted = fitted.reshape(NAUX, NLMO, DOM)
    norm_scale = NAUX ** -0.5
    energy = orbital_energy.astype(jnp.float32)
    coupling_wide = coupling.astype(jnp.float32)

    def owner(packed):
        wanted, slots, live_count = packed
        sources = jnp.arange(N_PAIR, dtype=jnp.int32)[:, None] * LMO_DEV
        ident = (sources + wanted).reshape(-1).astype(jnp.int32)
        orbits = ident[slots]
        left_ids = orbits[0::2]
        right_ids = orbits[1::2]
        left_rows = fitted[:, left_ids, :].astype(jnp.float32)
        right_rows = fitted[:, right_ids, :].astype(jnp.float32)
        exchange = jnp.einsum("qsa,qsb->sab", left_rows, right_rows) * norm_scale
        rounded = lax.optimization_barrier(exchange.astype(jnp.bfloat16)).astype(jnp.float32)
        weighted = jnp.einsum("sab,bc->sac", rounded, coupling_wide)
        denom = cabs_energy[None, None, :] - (energy[left_ids] + energy[right_ids])[:, None, None]
        live_mask = jnp.arange(PAIR_CAP, dtype=jnp.int32) < live_count
        return jnp.where(live_mask[:, None, None], weighted / denom, 0.0).astype(jnp.bfloat16)

    return lax.map(owner, (send_map, pair_slots, pair_count))
```

```python
import functools

import jax
import jax.numpy as jnp
from jax import lax
from jax.experimental import pallas as pl
from jax.experimental.pallas import tpu as pltpu
from jax.sharding import PartitionSpec as P


CHUNKS = 4
GROUP = 4


def pair_kernel(n_src, scale, meta_ref, loc_ref, *refs):
    sources = refs[:n_src]
    out_ref = refs[n_src]
    left, right, left_sem, right_sem = refs[n_src + 1 :]
    size = out_ref.shape[1]
    base, groups = meta_ref[0], meta_ref[1]

    def fetch(slot, row, buf, sem, place):
        where = loc_ref[row, slot]
        first = pl.multiple_of(loc_ref[row + 1, slot] * size, size)
        for at, source in enumerate(sources):

            @pl.when(where == at)
            def _():
                pltpu.make_async_copy(
                    source.at[pl.ds(first, size), :], buf.at[place], sem.at[place]
                ).start()

    def fetch_group(group):
        for u in range(GROUP):
            slot = base + group * GROUP + u
            place = lax.rem(group, 2) * GROUP + u
            fetch(slot, 0, left, left_sem, place)
            fetch(slot, 2, right, right_sem, place)

    out_ref[...] = jnp.zeros_like(out_ref)

    @pl.when(groups > 0)
    def _():
        fetch_group(0)

    def advance(group, carry):
        @pl.when(group + 1 < groups)
        def _():
            fetch_group(group + 1)

        first = lax.rem(group, 2) * GROUP
        for u in range(GROUP):
            for buf, sem in ((left, left_sem), (right, right_sem)):
                pltpu.make_async_copy(
                    sources[0].at[pl.ds(0, size), :], buf.at[first + u], sem.at[first + u]
                ).wait()
        for u in range(GROUP):
            product = lax.dot_general(
                left[first + u],
                right[first + u],
                (((1,), (1,)), ((), ())),
                preferred_element_type=jnp.float32,
            )
            out_ref[group * GROUP + u] = (product * scale).astype(out_ref.dtype)
        return carry

    lax.fori_loop(0, groups, advance, 0)


def pair_blocks(sources, meta, loc, share, domain, scale):
    rows = sources[0].shape[1]
    return pl.pallas_call(
        functools.partial(pair_kernel, len(sources), scale),
        out_shape=jax.ShapeDtypeStruct((share, domain, domain), jnp.bfloat16),
        in_specs=[pl.BlockSpec(memory_space=pltpu.SMEM)] * 2
        + [pl.BlockSpec(memory_space=pl.ANY)] * len(sources),
        out_specs=pl.BlockSpec(memory_space=pltpu.VMEM),
        scratch_shapes=[
            pltpu.VMEM((2 * GROUP, domain, rows), jnp.bfloat16),
            pltpu.VMEM((2 * GROUP, domain, rows), jnp.bfloat16),
            pltpu.SemaphoreType.DMA((2 * GROUP,)),
            pltpu.SemaphoreType.DMA((2 * GROUP,)),
        ],
        name="pair_blocks",
    )(meta, loc, *sources)


def times(panel, factor):
    return lax.dot_general(
        panel, factor, (((0,), (1,)), ((), ())), preferred_element_type=jnp.float32
    ).astype(jnp.bfloat16)


def fit_through_hubs(factor, pieces):
    me = lax.axis_index("fit")
    rows = factor.shape[0]
    lane = lax.axis_index("pair")
    slab = rows // lax.axis_size("pair")
    inward, inner, outward = [(0, 1), (3, 2)], [(1, 2), (2, 1)], [(1, 0), (2, 3)]
    is_hub = (me == 1) | (me == 2)
    order = jnp.array([[0, 0, 0, 0], [1, 0, 2, 3], [2, 3, 1, 0], [0, 0, 0, 0]], jnp.int32)[me]

    def blocks(matrix):
        parts = [lax.dynamic_slice_in_dim(matrix, order[i] * rows, rows, 1) for i in range(4)]
        return lax.optimization_barrier(jnp.concatenate(parts, axis=1))

    part = lax.dynamic_slice_in_dim(factor, lane * slab, slab, 0)
    part = lax.ppermute(part, "fit", inward)
    part = lax.optimization_barrier(jnp.where(is_hub, part, jnp.zeros_like(part)))
    served = lax.all_gather(part, "pair", axis=0, tiled=True)
    own_blocks = blocks(factor)
    served_blocks = blocks(served)
    fitted = []
    for piece in pieces:
        outer = lax.ppermute(piece, "fit", inward)
        near = lax.ppermute(piece, "fit", inner)
        far = lax.ppermute(outer, "fit", inner)
        panel = jnp.concatenate([piece, outer, near, far], axis=0)
        panel = lax.optimization_barrier(panel)
        end = lax.optimization_barrier(times(panel, served_blocks))
        given = lax.ppermute(end, "fit", outward)
        own = lax.optimization_barrier(times(panel, own_blocks))
        fitted.append(lax.optimization_barrier(jnp.where(is_hub, own, given)))
    return fitted


def fit_gathered(factor, pieces):
    return [times(lax.all_gather(piece, "fit", axis=0, tiled=True), factor) for piece in pieces]


def on_device(
    metric_factor,
    three_index,
    send_map,
    pair_slots,
    pair_count,
    orbital_energy,
    cabs_energy,
    coupling,
):
    domain = coupling.shape[0]
    orbitals = orbital_energy.shape[0]
    peers = send_map.shape[1]
    capacity = send_map.shape[2]
    slot_total = pair_slots.shape[1] // 2
    fit_size = lax.axis_size("fit")
    me = lax.axis_index("fit")
    share = slot_total // fit_size
    first_slot = me * share
    live_count = pair_count[0]
    scale = metric_factor.shape[1] ** (-0.5)
    group = orbitals // CHUNKS
    width = group * domain

    energy_src = lax.all_gather(orbital_energy, "pair", axis=0, tiled=True)
    peer_ids = jnp.broadcast_to(jnp.arange(peers, dtype=jnp.int32)[:, None], (peers, capacity))
    requests = send_map.reshape(peers, capacity)
    slots = pair_slots[0]
    picked = jnp.take(requests.reshape(-1), slots)
    origin = jnp.take(peer_ids.reshape(-1), slots)
    piece_of = picked // group
    row_of = origin * group + picked % group
    loc = jnp.stack([piece_of[0::2], row_of[0::2], piece_of[1::2], row_of[1::2]])
    energies = jnp.take(energy_src, origin * orbitals + picked).astype(jnp.float32)
    energy_sum = energies[0::2] + energies[1::2]
    energy_sum = lax.dynamic_slice_in_dim(energy_sum, first_slot, share, 0)
    loc, energy_sum = lax.optimization_barrier((loc, energy_sum))

    pieces = [three_index[:, c * width : (c + 1) * width] for c in range(CHUNKS)]
    fit = fit_through_hubs if fit_size == 4 else fit_gathered
    fitted = fit(metric_factor, pieces)
    sources = [lax.all_gather(block, "pair", axis=0, tiled=True) for block in fitted]

    def block_for(target):
        base = target * share
        live = jnp.clip(live_count - base, 0, share)
        meta = jnp.stack([base, (live + GROUP - 1) // GROUP]).astype(jnp.int32)
        return pair_blocks(sources, meta, loc, share, domain, scale)

    received = []
    for shift in sorted(range(1, fit_size), key=lambda d: abs(d - fit_size / 2)):
        block = block_for((me + shift) % fit_size)
        ring = [(i, (i + shift) % fit_size) for i in range(fit_size)]
        received.append(lax.ppermute(block, "fit", ring))
    total = block_for(me).astype(jnp.float32)
    for block in received:
        total = total + block.astype(jnp.float32)
    exchange = total.astype(jnp.bfloat16)

    weighted = jnp.einsum("sab,bc->sac", exchange, coupling, preferred_element_type=jnp.float32)
    denom = cabs_energy[None, None, :] - energy_sum[:, None, None]
    live_mask = first_slot + jnp.arange(share, dtype=jnp.int32) < live_count
    projected = jnp.where(live_mask[:, None, None], weighted / denom, 0.0).astype(jnp.bfloat16)
    return projected.reshape(1, share, domain, weighted.shape[2])


def solution(mesh):
    in_specs = (
        P("fit", None),
        P("fit", "pair"),
        P("pair", None, None),
        P("pair", None),
        P("pair"),
        P("pair"),
        P(),
        P(),
    )
    out_specs = P("pair", "fit", None, None)

    return jax.shard_map(
        on_device, mesh=mesh, in_specs=in_specs, out_specs=out_specs, check_vma=False
    )
```
